32 devices in a mesh: dp: 8 (over z, y), tensor: 4 (over x, core).
Axes of the slice: x: 2, y: 2, z: 4, core: 2. Of those that a mesh axis runs over, the one named last changes fastest.
Arguments:
- tokens: bfloat16 [16384, 4096], P('dp', 'tensor'), may hold values from -6 to 6
- cotangent: bfloat16 [16384, 1536], P('dp', 'tensor'), may hold values from -0.059814453 to 0.059814453
- seg_start: int32 [8, 2], P('dp'), may hold values from 0 to 1024, as said below
- seg_length: int32 [8, 2], P('dp'), may hold values from 0 to 1024, as said below
Outputs:
- weight_grad: float32 [4096, 2, 1536], P('dp', None, 'tensor')
The draws below stay inside these ranges and needn't reach their ends.
Inputs may be any that keep to these rules, and one draw needn't show every extreme that they name: Within each index of dp the 2 segments lie in expert order, packed from row 0 without gaps: seg_start is the running sum of seg_length before each expert. `seg_length`: each length is at most 1024; in every draw some expert on some index of dp has exactly 1024 rows. Rows after the last segment belong to no expert.
All inputs are finite; a program needn't handle non-finite values.
Results may differ from the reference program's by a relative error of at most 0.0003.
Values may be sent and summed in bfloat16 or wider, within the bound.
No kernel may reach another device: no remote copies, remote signals or barrier semaphores. Data moves between devices by JAX's collectives and lax.ppermute only.
A program may use at most 128 MiB of HBM per device.

```python
import jax
import jax.numpy as jnp
from jax import lax

D = 4096
FF = 1536
E_W = 2
CAP = 1024
TOKENS = 16384
N_DP = 8


def segment_bounds(key):
    keys = jax.random.split(jax.random.fold_in(key, 7), 4)
    load = jax.random.randint(keys[0], (N_DP, 1), 1, 5)
    lower = load * CAP // 8
    upper = load * CAP // 4 + 1
    draws = jax.random.randint(keys[1], (N_DP, E_W), 0, 1 << 30)
    length = lower + draws % (upper - lower)
    busy_device = jax.random.randint(keys[2], (), 0, N_DP)
    busy_expert = jax.random.randint(keys[3], (), 0, E_W)
    hit = (jnp.arange(N_DP)[:, None] == busy_device) & (jnp.arange(E_W)[None, :] == busy_expert)
    length = jnp.where(hit, CAP, length)
    start = jnp.cumsum(length, axis=1) - length
    return (start.astype(jnp.int32), length.astype(jnp.int32))


def draw_seg_start(key, part):
    return segment_bounds(key)[0]


def draw_seg_length(key, part):
    return segment_bounds(key)[1]


def with_spikes(values, rng, source, target, shards_of, factor):
    owner, partner = [(jnp.arange(values.shape[axis_at]) // (values.shape[axis_at] // shards_of)).reshape([-1 if axis == axis_at else 1 for axis in range(values.ndim)]) for axis_at in (source, target)]
    chosen = jax.random.permutation(rng, shards_of)[partner]
    strong = (owner == chosen) | (owner == (partner + shards_of // 2) % shards_of)
    return jnp.where(strong, factor * values, values)


def level_of(own_key, extent, shards, low, high):
    factor_of = 1.0
    for position, parts in shards:
        steps = jax.random.uniform(jax.random.fold_in(jax.random.fold_in(own_key, 6), position), (parts,), jnp.float32, low / len(shards), high / len(shards))
        factor_of = factor_of * jnp.repeat(jnp.exp(steps), extent[position] // parts).reshape((-1,) + (1,) * (len(extent) - 1 - position))
    return factor_of


def noise(key, extent, scale, bound, cuts=(), kind=jnp.bfloat16):
    values = jax.random.normal(key, extent, jnp.float32) * scale
    if len(cuts) > 0:
        values = level_of(key, extent, cuts, -0.22, 0.18) * values
    return jnp.clip(values, min=-bound, max=bound).astype(kind)


def bell_draw_with(stream_key, shape, width, bound, cuts, heavy, kind=jnp.bfloat16):
    drawn = width * jax.random.normal(stream_key, shape, jnp.float32)
    if cuts:
        drawn = drawn * level_of(stream_key, shape, cuts, -0.22, 0.18)
    return jnp.clip(with_spikes(drawn, jax.random.fold_in(stream_key, 3), *heavy), -bound, bound).astype(kind)


def setup_inputs(seed: int = 0) -> dict:
    splits = jax.random.split(jax.random.key(seed), 5)
    tokens = bell_draw_with(splits[0], (TOKENS, D), 1.0, 6.0, ((0, 8), (1, 4)), (0, 1, 8, 2.0))
    cotangent = noise(splits[1], (TOKENS, FF), 0.01, 0.059814453, ((0, 8), (1, 4)))
    seg_start = draw_seg_start(jax.random.fold_in(splits[4], 71), 0)
    seg_length = draw_seg_length(jax.random.fold_in(splits[4], 71), 0)
    return dict(tokens=tokens, cotangent=cotangent, seg_start=seg_start, seg_length=seg_length)


def reference(tokens, cotangent, seg_start, seg_length):
    tok = E_W * CAP

    def peer(total, index):
        rows_x = lax.dynamic_slice_in_dim(tokens, index * tok, tok, 0)
        rows_g = lax.dynamic_slice_in_dim(cotangent, index * tok, tok, 0)
        terms = []
        for expert in range(E_W):
            start = seg_start[index, expert].astype(jnp.int32)
            length = seg_length[index, expert].astype(jnp.int32)
            first = jnp.minimum(start, tok - CAP).astype(jnp.int32)
            rows = first + jnp.arange(CAP, dtype=jnp.int32)
            keep = (rows >= start) & (rows < start + length)
            block_x = lax.dynamic_slice_in_dim(rows_x, first, CAP, 0)
            block_g = lax.dynamic_slice_in_dim(rows_g, first, CAP, 0)
            block_g = jnp.where(keep[:, None], block_g, jnp.zeros_like(block_g))
            terms.append(jnp.dot(block_x.T, block_g, preferred_element_type=jnp.float32))
        return total + jnp.stack(terms, 1), None

    start_total = jnp.zeros((D, E_W, FF), jnp.float32)
    total, unused = lax.scan(peer, start_total, jnp.arange(N_DP, dtype=jnp.int32))
    return total
```

```python
import jax
import jax.numpy as jnp
from jax import lax
from jax.sharding import PartitionSpec as P

CHUNKS = 4
TOP = 15.0
TAIL = 16
HALF = True


def swap(n, bit):
    return [(i, i ^ bit) for i in range(n)]


def coded_pieces(pieces):
    peak = jnp.max(jnp.abs(jnp.stack(pieces)))
    power = jnp.ceil(jnp.log2(jnp.maximum(peak, 1e-30))) + 1.0
    tail = jnp.full((TAIL, pieces[0].shape[1]), power, jnp.float32)
    scale = jnp.exp2(TOP - power)
    return [jnp.concatenate([p * scale, tail], 0).astype(jnp.float16) for p in pieces]


def decoded(coded):
    coded = coded.astype(jnp.float32)
    return coded[:-TAIL] * jnp.exp2(coded[-1:] - TOP)


def spread(block, n_tensor):
    got = {0: block}
    bit = n_tensor // 2
    while bit:
        for k, value in list(got.items()):
            got[k ^ bit] = lax.ppermute(value, "tensor", swap(n_tensor, bit))
        bit //= 2
    return got


def solution(mesh):
    n_dp, n_tensor = mesh.shape["dp"], mesh.shape["tensor"]
    pair = swap(n_dp, 1)
    outer = n_dp // 2
    groups = [[2 * o + i for o in range(outer)] for i in range(2)]

    def per_device(tokens, cotangent, seg_start, seg_length):
        experts = seg_start.shape[1]
        assert experts == 2
        cap = tokens.shape[0] // experts
        width = tokens.shape[1]
        hidden = cotangent.shape[1]
        mine = lax.axis_index("dp") % 2
        here = lax.axis_index("tensor")
        pieces = max(outer // n_tensor, 1)
        part = width // (pieces * 2 * CHUNKS)

        def bounds(expert):
            start = lax.dynamic_index_in_dim(seg_start[0], expert, 0, False)
            length = lax.dynamic_index_in_dim(seg_length[0], expert, 0, False)
            return jnp.minimum(start, tokens.shape[0] - cap), start, start + length

        def columns(expert, c):
            first = bounds(expert)[0]
            step = width // (2 * pieces)
            cols = [
                lax.dynamic_slice(tokens, (first, j * step + c * part), (cap, part))
                for j in range(2 * pieces)
            ]
            return jnp.concatenate(cols, 1)

        def grads(expert):
            first, start, end = bounds(expert)
            rows = first + jnp.arange(cap, dtype=jnp.int32)
            keep = (rows >= start) & (rows < end)
            g = lax.dynamic_slice_in_dim(cotangent, first, cap, 0)
            return jnp.where(keep[:, None], g, jnp.zeros_like(g))

        x_in = []
        for c in range(CHUNKS):
            x_in.append(lax.ppermute(columns(1 - mine, c), "dp", pair))
        g_own = grads(mine)
        g_in = lax.ppermute(grads(1 - mine), "dp", pair)
        g = jnp.concatenate([g_own, g_in], 0)
        kept, sent = [], []
        for c in range(CHUNKS):
            got = spread(jnp.concatenate([columns(mine, c), x_in[c]], 0), n_tensor)
            dims = (((0,), (0,)), ((), ()))
            terms = [
                lax.dot_general(got[k], g, dims, preferred_element_type=jnp.float32)
                for k in range(n_tensor)
            ]
            if HALF and outer == n_tensor:
                stacked = jnp.stack(terms)
                away = (lax.axis_index("dp") // 2) ^ here
                split = [
                    lax.dynamic_index_in_dim(stacked, away ^ d, 0, False) for d in range(outer)
                ]
                coded = coded_pieces(split[1:])
                piece = split[0]
                for d in range(1, outer):
                    moved = lax.ppermute(coded[d - 1], "dp", swap(n_dp, 2 * d))
                    piece += decoded(moved)
            else:
                total = jnp.zeros((n_tensor,) + terms[0].shape, jnp.float32)
                for k in range(n_tensor):
                    total = lax.dynamic_update_index_in_dim(total, terms[k], here ^ k, 0)
                total = total.reshape(outer, -1, hidden)
                piece = lax.psum_scatter(
                    total, "dp", scatter_dimension=0, axis_index_groups=groups, tiled=True
                )
            piece = piece.reshape(2, part, hidden)
            kept.append(lax.dynamic_index_in_dim(piece, mine, 0, False))
            out = lax.dynamic_index_in_dim(piece, 1 - mine, 0, False)
            sent.append(lax.ppermute(out, "dp", pair))
        kept = jnp.concatenate(kept, 0)
        sent = jnp.concatenate(sent, 0)
        first = jnp.where(mine == 0, kept, sent)
        second = jnp.where(mine == 0, sent, kept)
        return jnp.stack([first, second], 1)

    in_specs = (P("dp", "tensor"), P("dp", "tensor"), P("dp", None), P("dp", None))
    out_specs = P("dp", None, "tensor")

    return jax.shard_map(
        per_device, mesh=mesh, in_specs=in_specs, out_specs=out_specs, check_vma=False
    )
```
